8 devices in a mesh: dp: 2 (over z, y), ep: 4 (over x, core).
Axes of the slice: x: 2, y: 2, z: 1, core: 2. Of those that a mesh axis runs over, the one named last changes fastest.
Arguments:
- hidden: bfloat16 [16384, 1024], P(('dp', 'ep'))
- grad_out: bfloat16 [16384, 1024], P(('dp', 'ep'))
- expert_ids: int32 [16384, 2], P(('dp', 'ep'))
- norm_gain: float32 [1024], replicated
- w_router: float32 [1024, 32], replicated
- w_gate: bfloat16 [32, 1024, 2816], P('ep')
- w_up: bfloat16 [32, 1024, 2816], P('ep')
- w_down: bfloat16 [32, 2816, 1024], P('ep')
Outputs:
- output 1: bfloat16 [16384, 1024], P(('dp', 'ep'))
- output 2: float32 [], replicated
- output 3: bfloat16 [16384, 1024], P(('dp', 'ep'))
- output 4: float32 [1024], replicated
- output 5: float32 [1024, 32], replicated
- output 6: bfloat16 [32, 1024, 2816], P('ep')
- output 7: bfloat16 [32, 1024, 2816], P('ep')
- output 8: bfloat16 [32, 2816, 1024], P('ep')
All inputs are finite; a program needn't handle non-finite values.
Results may differ from the reference program's by a relative error of at most 0.0152594.
Values are sent between devices in bfloat16 or wider.
A program may use at most 1.25 GiB of HBM per device.

```python
import functools
import jax
import jax.numpy as jnp
from jax import lax

D = 1024
FF = 2816
EXPERTS = 32
TOK = 2048
DEVICES = 8
CAP = 4 * TOK // EXPERTS
ROWS_EXP = DEVICES * CAP
S_ALL = TOK * DEVICES
EPS = 1e-6
AUX_COEF = 0.001


def draw_routes(key):
    key_order, key_shift, key_perm, key_swap = jax.random.split(key, 4)
    half_exp = EXPERTS // 2
    mean_load = 2 * TOK // EXPERTS
    shift = jax.random.randint(key_shift, (DEVICES, half_exp), 0, mean_load + 1)
    shift = shift.at[:, 0].set(mean_load)
    order = jax.vmap(lambda sub_key: jax.random.permutation(sub_key, EXPERTS))(jax.random.split(key_order, DEVICES))
    signed = jnp.concatenate([shift, -shift], axis=1)
    expert_range = jnp.arange(EXPERTS, dtype=jnp.int32)
    loads = mean_load + jnp.sum(signed[:, :, None] * (order[:, :, None] == expert_range).astype(jnp.int32), axis=1)
    bounds = jnp.cumsum(loads, axis=1)
    positions = jnp.arange(2 * TOK, dtype=jnp.int32)
    listed = jax.vmap(lambda bound_row: jnp.searchsorted(bound_row, positions, side="right"))(bounds).astype(jnp.int32)
    token_order = jax.vmap(lambda sub_key: jax.random.permutation(sub_key, TOK))(jax.random.split(key_perm, DEVICES))
    first = jnp.take_along_axis(listed[:, :TOK], token_order, axis=1)
    second = jnp.take_along_axis(listed[:, TOK:], token_order, axis=1)
    swap = jax.random.randint(key_swap, (DEVICES, TOK), 0, 2) == 1
    id_first = jnp.where(swap, second, first)
    id_second = jnp.where(swap, first, second)
    return jnp.stack([id_first, id_second], axis=-1).reshape(DEVICES * TOK, 2).astype(jnp.int32)


def setup_inputs(seed: int = 0) -> dict:
    key = jax.random.key(seed)
    keys = jax.random.split(key, 8)
    expert_ids = draw_routes(keys[0])
    w_router = jax.random.normal(keys[1], (D, EXPERTS), jnp.float32) * D ** -0.5
    col_dir = w_router * lax.rsqrt(jnp.mean(w_router * w_router, axis=0, keepdims=True))
    chosen = jnp.sum((expert_ids[:, :, None] == jnp.arange(EXPERTS, dtype=jnp.int32)).astype(jnp.float32), axis=1)
    boost = jnp.dot(chosen, col_dir.T, preferred_element_type=jnp.float32)
    hidden = jax.random.normal(keys[2], (S_ALL, D), jnp.float32) + (2.5 * D ** -0.5) * boost
    grad_out = jax.random.normal(keys[3], (S_ALL, D), jnp.float32)
    norm_gain = 1.0 + 0.3 * jax.random.normal(keys[4], (D,), jnp.float32)
    w_gate = jax.random.normal(keys[5], (EXPERTS, D, FF), jnp.float32) * D ** -0.5
    w_up = jax.random.normal(keys[6], (EXPERTS, D, FF), jnp.float32) * D ** -0.5
    w_down = jax.random.normal(keys[7], (EXPERTS, FF, D), jnp.float32) * (2.0 * FF ** -0.5)
    return {"hidden": hidden.astype(jnp.bfloat16), "grad_out": grad_out.astype(jnp.bfloat16), "expert_ids": expert_ids, "norm_gain": norm_gain, "w_router": w_router, "w_gate": w_gate.astype(jnp.bfloat16), "w_up": w_up.astype(jnp.bfloat16), "w_down": w_down.astype(jnp.bfloat16)}


def bf16_trip(value):
    return value.astype(jnp.bfloat16).astype(jnp.float32)


def route_tables(expert_ids, n_exp, capacity):
    flat_ids = expert_ids.reshape(-1)
    n_choice = flat_ids.shape[0]
    one_hot = (flat_ids[:, None] == jnp.arange(n_exp, dtype=jnp.int32)[None, :]).astype(jnp.int32)
    running = jnp.cumsum(one_hot, axis=0) - 1
    dest_rows = flat_ids * capacity + jnp.sum(running * one_hot, axis=1)
    slot_owner = jnp.full((n_exp * capacity,), n_choice, jnp.int32).at[dest_rows].set(jnp.arange(n_choice, dtype=jnp.int32))
    return dest_rows, slot_owner, jnp.sum(one_hot, axis=0)


def expert_ffn(operands):
    rows, gate_w, up_w, down_w = operands
    h_gate = bf16_trip(jnp.dot(rows, gate_w.astype(jnp.float32), preferred_element_type=jnp.float32))
    h_up = bf16_trip(jnp.dot(rows, up_w.astype(jnp.float32), preferred_element_type=jnp.float32))
    act_rows = bf16_trip(jax.nn.silu(h_gate) * h_up)
    return bf16_trip(jnp.dot(act_rows, down_w.astype(jnp.float32), preferred_element_type=jnp.float32))


def forward_pass(hidden, norm_gain, w_router, w_gate, w_up, w_down, expert_ids):
    dest_rows, slot_owner, loads = route_tables(expert_ids, EXPERTS, ROWS_EXP)
    choice_hot = (expert_ids[:, :, None] == jnp.arange(EXPERTS, dtype=jnp.int32)).astype(jnp.float32)
    x_f32 = hidden.astype(jnp.float32)
    inv_rms = lax.rsqrt(jnp.mean(x_f32 * x_f32, axis=-1, keepdims=True) + EPS)
    x_norm = bf16_trip(x_f32 * inv_rms * norm_gain)
    logits = jnp.dot(x_norm, w_router, preferred_element_type=jnp.float32)
    router_probs = jax.nn.softmax(logits, axis=-1)
    gate_vals = jnp.sum(router_probs[:, None, :] * choice_hot, axis=-1)
    rows = bf16_trip(jnp.take(x_norm, slot_owner // 2, axis=0, mode="fill", fill_value=0))
    exp_out = lax.map(jax.checkpoint(expert_ffn), (rows.reshape(EXPERTS, ROWS_EXP, D), w_gate, w_up, w_down))
    picked = jnp.take(exp_out.reshape(EXPERTS * ROWS_EXP, D), dest_rows, axis=0).reshape(S_ALL, 2, D)
    out_hidden = (x_f32 + jnp.sum(gate_vals[:, :, None] * picked, axis=1)).astype(jnp.bfloat16)
    load_frac = loads.astype(jnp.float32) / (2 * S_ALL)
    aux_loss = AUX_COEF * EXPERTS * jnp.sum(load_frac * jnp.mean(router_probs, axis=0))
    return out_hidden, aux_loss


def reference(hidden, grad_out, expert_ids, norm_gain, w_router, w_gate, w_up, w_down):
    forward_fn = functools.partial(forward_pass, expert_ids=expert_ids)
    (out_hidden, aux_loss), pullback = jax.vjp(forward_fn, hidden, norm_gain, w_router, w_gate, w_up, w_down)
    all_grads = pullback((grad_out, jnp.ones_like(aux_loss)))
    return (out_hidden, aux_loss, all_grads[0], all_grads[1], all_grads[2], all_grads[3], all_grads[4], all_grads[5])
```

```python
import functools

import jax
import jax.numpy as jnp
from jax import lax
from jax.experimental import pallas as pl
from jax.experimental.pallas import tpu as pltpu
from jax.sharding import PartitionSpec as P


EPS = 1e-6
AUX_COEF = 0.001
TM = 256
CF = 256
SUB = 16
GROUP_SIZES = (3, 2, 2, 1)


def gather_kernel(scaled, src_ref, rows_ref, table_ref, tok_ref, gate_ref, out_ref):
    @pl.when(pl.program_id(1) * TM < rows_ref[pl.program_id(0)])
    def _():
        n_tok = table_ref.shape[0]
        tok = tok_ref[...]
        lane = lax.broadcasted_iota(jnp.int32, tok.shape, 1).astype(jnp.float32)
        hot = jnp.concatenate([jnp.where(tok == lane + float(j), 1.0, 0.0).astype(jnp.bfloat16) for j in range(0, n_tok, 128)], axis=1)
        got = jnp.dot(hot, table_ref[...], preferred_element_type=jnp.float32)
        if scaled:
            got = got * gate_ref[:, 0:1]
        out_ref[...] = got.astype(jnp.bfloat16)


def gather_rows(scaled, src_ids, n_rows, table, tok, gate, n_tok):
    n_src, cap = tok.shape[0], tok.shape[1]
    width = table.shape[1]
    col = pl.BlockSpec((None, TM, 128), lambda k, r, *_: (k, r, 0))
    return pl.pallas_call(
        functools.partial(gather_kernel, scaled),
        out_shape=jax.ShapeDtypeStruct((n_src, cap, width), jnp.bfloat16),
        grid_spec=pltpu.PrefetchScalarGridSpec(
            num_scalar_prefetch=2,
            grid=(n_src, cap // TM),
            in_specs=[pl.BlockSpec((n_tok, width), lambda k, r, src, *_: (src[k], 0)), col, col],
            out_specs=pl.BlockSpec((None, TM, width), lambda k, r, *_: (k, r, 0)),
        ),
        compiler_params=pltpu.CompilerParams(dimension_semantics=("arbitrary", "arbitrary"), vmem_limit_bytes=40000000),
        cost_estimate=pl.CostEstimate(flops=n_src * cap * n_tok * width, bytes_accessed=n_src * (cap + n_tok) * width * 2, transcendentals=0),
        name="gather_rows",
    )(src_ids, n_rows, table, tok, gate)


def expert_kernel(e0, n_src, n_own, n_chunk, cnt_ref, soff_ref, off_ref, xa_hbm, xb_hbm, dy_hbm, wg_ref, wu_ref, wd_ref, _gg, _gu, _gd, gg_ref, gu_ref, gd_ref, *refs):
    out_hbm, refs = refs[:n_own], refs[n_own:]
    xbuf, dobuf, xt, o_acc, dx_acc, gxs, gds, ost, dxst, load_sem, out_sem = refs
    le = pl.program_id(0)
    c = pl.program_id(1)
    n_e = pl.num_programs(0)
    e = e0 + le
    slot = lax.rem(le, 2)
    half = xa_hbm.shape[2]
    bf16 = jnp.bfloat16
    f32 = jnp.float32

    def loads(expert, slot_i, start):
        for s in range(n_src):
            n = pl.multiple_of(cnt_ref[expert, s], SUB)

            @pl.when(n > 0)
            def _():
                src = pl.ds(pl.multiple_of(soff_ref[expert, s], SUB), n)
                dst = pl.ds(pl.multiple_of(off_ref[expert, s], SUB), n)
                copies = (
                    pltpu.make_async_copy(xa_hbm.at[s, src], xbuf.at[slot_i, dst, pl.ds(0, half)], load_sem.at[0]),
                    pltpu.make_async_copy(xb_hbm.at[s, src], xbuf.at[slot_i, dst, pl.ds(half, half)], load_sem.at[2]),
                    pltpu.make_async_copy(dy_hbm.at[s, src], dobuf.at[slot_i, dst], load_sem.at[1]),
                )
                for cp in copies:
                    if start:
                        cp.start()
                    else:
                        cp.wait()

    own_rows = off_ref[e, n_own]
    tot_rows = off_ref[e, n_src]
    nt_own = lax.div(own_rows + (TM - 1), TM)
    nt = jnp.maximum(lax.div(tot_rows + (TM - 1), TM), nt_own)

    @pl.when((le == 0) & (c == 0))
    def _():
        loads(e, slot, True)

    @pl.when(c == 0)
    def _():
        loads(e, slot, False)

        @pl.when(nt > 0)
        def _():
            rows = pl.ds(pl.multiple_of((nt - 1) * TM, TM), TM)
            valid = ((nt - 1) * TM + lax.broadcasted_iota(jnp.int32, (TM, 1), 0)) < tot_rows
            for buf in (xbuf, dobuf):
                buf[slot, rows, :] = jnp.where(valid, buf[slot, rows, :].astype(f32), 0.0).astype(bf16)

        def prep(r, _):
            xt[r] = xbuf[slot, pl.ds(pl.multiple_of(r * TM, TM), TM), :].T
            return 0

        lax.fori_loop(0, nt, prep, 0)

    @pl.when((c == 1) & (le + 1 < n_e))
    def _():
        loads(e + 1, 1 - slot, True)

    @pl.when(nt == 0)
    def _():
        gxs[...] = jnp.zeros_like(gxs)
        gds[...] = jnp.zeros_like(gds)

    nt_dims = (((1,), (1,)), ((), ()))
    tn_dims = (((0,), (0,)), ((), ()))

    def tile(r, n_tile, own):
        rows = pl.ds(pl.multiple_of(r * TM, TM), n_tile * TM)
        x = xbuf[slot, rows, :]
        d_o = dobuf[slot, rows, :]
        hg = jnp.dot(x, wg_ref[...], preferred_element_type=f32).astype(bf16).astype(f32)
        hu = jnp.dot(x, wu_ref[...], preferred_element_type=f32).astype(bf16).astype(f32)
        da = lax.dot_general(d_o, wd_ref[...], nt_dims, preferred_element_type=f32).astype(bf16).astype(f32)
        sig = jax.nn.sigmoid(hg)
        silu = hg * sig
        act = (silu * hu).astype(bf16)
        dhu = (da * silu).astype(bf16)
        dhg = (da * hu * sig * (1.0 + hg * (1.0 - sig))).astype(bf16)
        both = jnp.concatenate([dhg, dhu], axis=1)
        if own:
            new = c == 0
            o_acc[rows, :] = jnp.where(new, 0.0, o_acc[rows, :]) + jnp.dot(act, wd_ref[...], preferred_element_type=f32)
            w_both = jnp.concatenate([wg_ref[...], wu_ref[...]], axis=1)
            dx_acc[rows, :] = jnp.where(new, 0.0, dx_acc[rows, :]) + lax.dot_general(both, w_both, nt_dims, preferred_element_type=f32)
        xtr = xt[r] if n_tile == 1 else jnp.concatenate([xt[r + i] for i in range(n_tile)], axis=1)
        gxs[...] = jnp.where(r == 0, 0.0, gxs[...]) + jnp.dot(xtr, both, preferred_element_type=f32)
        gds[...] = jnp.where(r == 0, 0.0, gds[...]) + lax.dot_general(act, d_o, tn_dims, preferred_element_type=f32)

    def run(lo, n, own):
        pairs = lax.div(n, 2)

        def pair(i, _):
            tile(lo + 2 * i, 2, own)
            return 0

        def single(i, _):
            tile(lo + 2 * pairs + i, 1, own)
            return 0

        lax.fori_loop(0, pairs, pair, 0)
        lax.fori_loop(0, n - 2 * pairs, single, 0)

    run(0, nt_own, True)
    run(nt_own, nt - nt_own, False)
    gg_ref[...] = gxs[:, :CF].astype(bf16)
    gu_ref[...] = gxs[:, CF:].astype(bf16)
    gd_ref[...] = gds[...].astype(bf16)

    @pl.when(c == n_chunk - 1)
    def _():
        def cast(r, _):
            rows = pl.ds(pl.multiple_of(r * TM, TM), TM)
            ost[rows, :] = o_acc[rows, :].astype(bf16)
            dxst[rows, :] = dx_acc[rows, :].astype(bf16)
            return 0

        lax.fori_loop(0, nt_own, cast, 0)
        for start in (True, False):
            for s in range(n_own):
                n = pl.multiple_of(cnt_ref[e, s], SUB)

                @pl.when(n > 0)
                def _():
                    src = pl.ds(pl.multiple_of(off_ref[e, s], SUB), n)
                    copies = (
                        pltpu.make_async_copy(ost.at[src], out_hbm[s].at[0, le, pl.ds(0, n)], out_sem.at[0]),
                        pltpu.make_async_copy(dxst.at[src], out_hbm[s].at[1, le, pl.ds(0, n)], out_sem.at[1]),
                    )
                    for cp in copies:
                        if start:
                            cp.start()
                        else:
                            cp.wait()


def run_experts(e0, n_e, cnt, soff, off, x_src, dy_src, seg_cap, w_gate, w_up, w_down, prev):
    n_src, cap, width = dy_src.shape
    n_loc = w_gate.shape[0]
    n_own = n_src // 2
    ff = w_gate.shape[2]
    n_chunk = ff // CF
    own_cap = n_own * seg_cap
    bf16 = jnp.bfloat16
    f32 = jnp.float32
    col_spec = pl.BlockSpec((None, width, CF), lambda i, c, *_: (e0 + i, 0, c))
    row_spec = pl.BlockSpec((None, CF, width), lambda i, c, *_: (e0 + i, c, 0))
    any_spec = pl.BlockSpec(memory_space=pl.ANY)
    first = prev is None
    if first:
        prev = (jnp.zeros((8, 128), bf16),) * 3
    out_shape = (
        jax.ShapeDtypeStruct((n_loc, width, ff), bf16),
        jax.ShapeDtypeStruct((n_loc, width, ff), bf16),
        jax.ShapeDtypeStruct((n_loc, ff, width), bf16),
    ) + (jax.ShapeDtypeStruct((2, n_e, seg_cap, width), bf16),) * n_own
    rows_est = n_e * cap // 2
    n_in = 9
    return pl.pallas_call(
        functools.partial(expert_kernel, e0, n_src, n_own, n_chunk),
        out_shape=out_shape,
        grid_spec=pltpu.PrefetchScalarGridSpec(
            num_scalar_prefetch=3,
            grid=(n_e, n_chunk),
            in_specs=[any_spec] * 3 + [col_spec, col_spec, row_spec] + [any_spec] * 3,
            out_specs=[col_spec, col_spec, row_spec] + [any_spec] * n_own,
            scratch_shapes=[
                pltpu.VMEM((2, cap, width), bf16),
                pltpu.VMEM((2, cap, width), bf16),
                pltpu.VMEM((cap // TM, width, TM), bf16),
                pltpu.VMEM((own_cap, width), f32),
                pltpu.VMEM((own_cap, width), f32),
                pltpu.VMEM((width, 2 * CF), f32),
                pltpu.VMEM((CF, width), f32),
                pltpu.VMEM((own_cap, width), bf16),
                pltpu.VMEM((own_cap, width), bf16),
                pltpu.SemaphoreType.DMA((3,)),
                pltpu.SemaphoreType.DMA((2,)),
            ],
        ),
        input_output_aliases={} if first else {n_in: 0, n_in + 1: 1, n_in + 2: 2},
        compiler_params=pltpu.CompilerParams(dimension_semantics=("arbitrary", "arbitrary"), vmem_limit_bytes=64000000),
        cost_estimate=pl.CostEstimate(flops=2 * 9 * rows_est * width * ff, bytes_accessed=n_e * width * ff * 12, transcendentals=0),
        name="experts",
    )(cnt, soff, off, *x_src, dy_src, w_gate, w_up, w_down, *prev)


def solution(mesh):
    n_dp, n_ep = mesh.shape["dp"], mesh.shape["ep"]
    n_dev = n_dp * n_ep
    all_axes = ("dp", "ep")

    def local_body(hidden, grad_out, expert_ids, norm_gain, w_router, w_gate, w_up, w_down):
        n_tok, width = hidden.shape
        n_exp = w_router.shape[1]
        n_loc = n_exp // n_ep
        capacity = 4 * n_tok // n_exp
        total_tok = n_tok * n_dev
        f32 = jnp.float32
        d_ix, e_ix = lax.axis_index("dp"), lax.axis_index("ep")

        dy_all = lax.all_gather(grad_out, all_axes, axis=0, tiled=True)

        x_f32 = hidden.astype(f32)
        inv_rms = lax.rsqrt(jnp.mean(x_f32 * x_f32, axis=-1, keepdims=True) + EPS)
        x_hat = x_f32 * inv_rms
        x_norm = (x_hat * norm_gain).astype(jnp.bfloat16)
        half = width // 2
        xa_all = lax.all_gather(x_norm[:, :half], all_axes, axis=0, tiled=True)
        xb_all = lax.all_gather(x_norm[:, half:], all_axes, axis=0, tiled=True)
        xn_f32 = x_norm.astype(f32)
        choice_hot = (expert_ids[:, :, None] == jnp.arange(n_exp, dtype=jnp.int32)).astype(f32)
        router_probs = jax.nn.softmax(jnp.dot(xn_f32, w_router, preferred_element_type=f32), axis=-1)
        gate_vals = jnp.sum(router_probs[:, None, :] * choice_hot, axis=-1)

        flat_ids = expert_ids.reshape(-1)
        one_hot = (flat_ids[:, None] == jnp.arange(n_exp, dtype=jnp.int32)[None, :]).astype(jnp.int32)
        running = jnp.cumsum(one_hot, axis=0) - 1
        dest_rows = flat_ids * capacity + jnp.sum(running * one_hot, axis=1)
        counts = jnp.sum(one_hot, axis=0)
        tokens = lax.broadcasted_iota(f32, (n_tok, 2), 0).reshape(-1)
        pair = jnp.stack([tokens, gate_vals.reshape(-1)], axis=1)
        n_slot = n_exp * capacity
        owner_rows = n_loc * capacity
        padded = (counts + (SUB - 1)) // SUB * SUB
        per_owner = padded.reshape(n_ep, n_loc)
        seg_off = (jnp.cumsum(per_owner, axis=1) - per_owner + owner_rows * jnp.arange(n_ep, dtype=jnp.int32)[:, None]).reshape(-1)
        packed = jnp.sum((running + seg_off[None, :]) * one_hot, axis=1)
        slots = jnp.broadcast_to(jnp.array([-1.0, 0.0], f32), (n_slot, 2)).at[packed].set(pair, unique_indices=True)
        slot_tok = slots[:, 0]
        slot_gate = slots[:, 1]
        mine = jnp.concatenate([slot_tok, slot_gate, counts.astype(f32), jnp.sum(router_probs, axis=0), jnp.zeros((64,), f32)])
        table = lax.all_gather(mine, all_axes, axis=0, tiled=False)
        route_stats = jnp.sum(table[:, 2 * n_slot:2 * n_slot + 2 * n_exp], axis=0)
        load_frac = route_stats[:n_exp] / (2 * total_tok)
        aux_loss = AUX_COEF * n_exp * jnp.sum(load_frac * route_stats[n_exp:] / total_tok)

        src_ids = [lax.rem(d_ix + k // n_ep, n_dp) * n_ep + lax.rem(e_ix + k % n_ep, n_ep) for k in range(n_dev)]
        mine_of = [lax.dynamic_index_in_dim(table, s, 0, keepdims=False) for s in src_ids]

        def cols(lo):
            part = jnp.stack([lax.dynamic_slice_in_dim(t, lo + e_ix * owner_rows, owner_rows, axis=0) for t in mine_of])
            return jnp.broadcast_to(part[..., None], (n_dev, owner_rows, 128))

        tok_col, gate_col = cols(0), cols(n_slot)
        cnt = jnp.stack([lax.dynamic_slice_in_dim(t, 2 * n_slot + e_ix * n_loc, n_loc, axis=0) for t in mine_of], axis=1).astype(jnp.int32)
        cnt = (cnt + (SUB - 1)) // SUB * SUB
        soff = jnp.cumsum(cnt, axis=0) - cnt
        off = jnp.concatenate([jnp.zeros((n_loc, 1), jnp.int32), jnp.cumsum(cnt, axis=1)], axis=1)
        n_rows = jnp.sum(cnt, axis=0)
        src_vec = jnp.stack(src_ids).astype(jnp.int32)
        dy_src = gather_rows(True, src_vec, n_rows, dy_all, tok_col, gate_col, n_tok)
        xa_all, dy_src = lax.optimization_barrier((xa_all, dy_src))
        xa_src = gather_rows(False, src_vec, n_rows, xa_all, tok_col, gate_col, n_tok)
        xb_all, xa_src = lax.optimization_barrier((xb_all, xa_src))
        x_src = (xa_src, gather_rows(False, src_vec, n_rows, xb_all, tok_col, gate_col, n_tok))

        prev = None
        backs = [[] for _ in range(n_ep)]
        e0 = 0
        for per in GROUP_SIZES:
            outs = run_experts(e0, per, cnt, soff, off, x_src, dy_src, capacity, w_gate, w_up, w_down, prev)
            prev = outs[:3]
            e0 += per
            for k in range(n_ep):
                sent = outs[3 + k]
                moved = sent
                if k > 0:
                    ring = [(i, (i + k) % n_ep) for i in range(n_ep)]
                    if e0 < n_loc:
                        moved = lax.ppermute(sent, "ep", ring)
                    else:
                        moved = (lax.ppermute(sent[0], "ep", ring), lax.ppermute(sent[1], "ep", ring))
                backs[k].append(moved)
        g_gate, g_up, g_down = prev
        back_rows = jnp.concatenate([b[0] for bk in backs for b in bk], axis=0).reshape(n_slot, width)
        d_back = jnp.concatenate([b[1] for bk in backs for b in bk], axis=0).reshape(n_slot, width)
        owner = dest_rows // owner_rows
        back_ix = (lax.rem(e_ix - owner + n_ep, n_ep) * owner_rows + lax.rem(dest_rows, owner_rows)).reshape(n_tok, 2)

        def picks(rows):
            return [rows.at[back_ix[:, j]].get(mode="promise_in_bounds").astype(f32) for j in range(2)]

        picked = picks(back_rows)
        out_hidden = (x_f32 + (gate_vals[:, 0:1] * picked[0] + gate_vals[:, 1:2] * picked[1])).astype(jnp.bfloat16)
        dy_f32 = grad_out.astype(f32)
        d_gates = jnp.stack([jnp.sum(dy_f32 * p, axis=-1) for p in picked], axis=1)
        d_xn_exp = picks(d_back)

        d_probs = jnp.sum(d_gates[:, :, None] * choice_hot, axis=1) + (AUX_COEF * n_exp / total_tok) * load_frac
        d_logits = router_probs * (d_probs - jnp.sum(router_probs * d_probs, axis=-1, keepdims=True))
        d_xnorm = jnp.einsum("te,de->td", d_logits, w_router) + d_xn_exp[0] + d_xn_exp[1]
        d_xnorm = d_xnorm.astype(jnp.bfloat16).astype(f32)
        scaled = d_xnorm * norm_gain
        grad_hidden = (inv_rms * (scaled - x_hat * jnp.mean(scaled * x_hat, axis=-1, keepdims=True)) + dy_f32).astype(jnp.bfloat16)
        grad_router = lax.psum(jnp.einsum("td,te->de", xn_f32, d_logits), all_axes)
        grad_gain = lax.psum(jnp.sum(d_xnorm * x_hat, axis=0), all_axes)
        return (out_hidden, aux_loss, grad_hidden, grad_gain, grad_router, g_gate, g_up, g_down)

    tok_spec = P(all_axes, None)
    w_spec = P("ep", None, None)
    return jax.shard_map(local_body, mesh=mesh, in_specs=(tok_spec, tok_spec, tok_spec, P(), P(), w_spec, w_spec, w_spec), out_specs=(tok_spec, P(), tok_spec, P(), P(), w_spec, w_spec, w_spec), check_vma=False)
```

```python
import functools

import jax
import jax.numpy as jnp
from jax import lax
from jax.experimental import pallas as pl
from jax.experimental.pallas import tpu as pltpu
from jax.sharding import PartitionSpec as P


EPS = 1e-6
AUX_COEF = 0.001
TM = 256
CF = 256
SUB = 16
GROUP_SIZES = (3, 2, 2, 1)


def first_gather_kernel(src_ref, rows_ref, table_ref, tok_ref, gate_ref, out_ref, hot_ref):
    @pl.when(pl.program_id(1) * TM < rows_ref[pl.program_id(0)])
    def _():
        n_tok = table_ref.shape[0]
        tok = tok_ref[...]
        lane = lax.broadcasted_iota(jnp.int32, tok.shape, 1).astype(jnp.float32)
        hot = jnp.concatenate([jnp.where(tok == lane + float(j), 1.0, 0.0).astype(jnp.bfloat16) for j in range(0, n_tok, 128)], axis=1)
        hot_ref[...] = hot
        got = jnp.dot(hot, table_ref[...], preferred_element_type=jnp.float32)
        out_ref[...] = (got * gate_ref[:, 0:1]).astype(jnp.bfloat16)


def next_gather_kernel(src_ref, rows_ref, table_ref, hot_ref, out_ref):
    @pl.when(pl.program_id(1) * TM < rows_ref[pl.program_id(0)])
    def _():
        out_ref[...] = jnp.dot(hot_ref[...], table_ref[...], preferred_element_type=jnp.float32).astype(jnp.bfloat16)


def gather_rows(src_ids, n_rows, table, n_tok, cap, hot=None, tok=None, gate=None):
    n_src = n_rows.shape[0]
    width = table.shape[1]

    def at(k, r, src, rows):
        return (k, jnp.minimum(r, jnp.maximum(lax.div(rows[k] + (TM - 1), TM) - 1, 0)), 0)

    col = pl.BlockSpec((None, TM, 128), at)
    hot_spec = pl.BlockSpec((None, TM, n_tok), at)
    row_spec = pl.BlockSpec((None, TM, width), at)
    table_spec = pl.BlockSpec((n_tok, width), lambda k, r, src, rows: (src[k], 0))
    row_shape = jax.ShapeDtypeStruct((n_src, cap, width), jnp.bfloat16)
    first = hot is None
    return pl.pallas_call(
        first_gather_kernel if first else next_gather_kernel,
        out_shape=(row_shape, jax.ShapeDtypeStruct((n_src, cap, n_tok), jnp.bfloat16)) if first else row_shape,
        grid_spec=pltpu.PrefetchScalarGridSpec(
            num_scalar_prefetch=2,
            grid=(n_src, cap // TM),
            in_specs=[table_spec, col, col] if first else [table_spec, hot_spec],
            out_specs=[row_spec, hot_spec] if first else row_spec,
        ),
        compiler_params=pltpu.CompilerParams(dimension_semantics=("arbitrary", "arbitrary"), vmem_limit_bytes=40000000),
        cost_estimate=pl.CostEstimate(flops=n_src * cap * n_tok * width, bytes_accessed=n_src * (cap + n_tok) * width * 2, transcendentals=0),
        name="gather_rows",
    )(src_ids, n_rows, table, *((tok, gate) if first else (hot,)))


def expert_kernel(e0, n_src, n_own, n_chunk, cnt_ref, soff_ref, off_ref, order_ref, xa_hbm, xb_hbm, dy_hbm, wg_ref, wu_ref, wd_ref, _gg, _gu, _gd, gg_ref, gu_ref, gd_ref, *refs):
    out_hbm, refs = refs[:n_own], refs[n_own:]
    xbuf, dobuf, xt, o_acc, dx_acc, gxs, gds, ost, dxst, load_sem, out_sem = refs
    le = pl.program_id(0)
    c = pl.program_id(1)
    n_e = pl.num_programs(0)
    e = e0 + le
    slot = lax.rem(le, 2)
    half = xa_hbm.shape[2]
    bf16 = jnp.bfloat16
    f32 = jnp.float32

    def loads(expert, slot_i, start):
        for s in range(n_src):
            n = pl.multiple_of(cnt_ref[expert, s], SUB)

            @pl.when(n > 0)
            def _():
                src = pl.ds(pl.multiple_of(soff_ref[expert, s], SUB), n)
                dst = pl.ds(pl.multiple_of(off_ref[expert, s], SUB), n)
                copies = (
                    pltpu.make_async_copy(xa_hbm.at[s, src], xbuf.at[slot_i, dst, pl.ds(0, half)], load_sem.at[0]),
                    pltpu.make_async_copy(xb_hbm.at[s, src], xbuf.at[slot_i, dst, pl.ds(half, half)], load_sem.at[2]),
                    pltpu.make_async_copy(dy_hbm.at[s, src], dobuf.at[slot_i, dst], load_sem.at[1]),
                )
                for cp in copies:
                    if start:
                        cp.start()
                    else:
                        cp.wait()

    def outputs(expert, place, start):
        for s in range(n_own):
            n = pl.multiple_of(cnt_ref[expert, s], SUB)

            @pl.when(n > 0)
            def _():
                src = pl.ds(pl.multiple_of(off_ref[expert, s], SUB), n)
                copies = (
                    pltpu.make_async_copy(ost.at[src], out_hbm[s].at[0, place, pl.ds(0, n)], out_sem.at[0]),
                    pltpu.make_async_copy(dxst.at[src], out_hbm[s].at[1, place, pl.ds(0, n)], out_sem.at[1]),
                )
                for cp in copies:
                    if start:
                        cp.start()
                    else:
                        cp.wait()

    own_rows = off_ref[e, n_own]
    tot_rows = off_ref[e, n_src]
    nt_own = lax.div(own_rows + (TM - 1), TM)
    nt = jnp.maximum(lax.div(tot_rows + (TM - 1), TM), nt_own)

    @pl.when((le == 0) & (c == 0))
    def _():
        loads(e, slot, True)

    @pl.when(c == 0)
    def _():
        loads(e, slot, False)

        @pl.when(nt > 0)
        def _():
            rows = pl.ds(pl.multiple_of((nt - 1) * TM, TM), TM)
            valid = ((nt - 1) * TM + lax.broadcasted_iota(jnp.int32, (TM, 1), 0)) < tot_rows
            for buf in (xbuf, dobuf):
                buf[slot, rows, :] = jnp.where(valid, buf[slot, rows, :].astype(f32), 0.0).astype(bf16)

        def prep(r, _):
            xt[r] = xbuf[slot, pl.ds(pl.multiple_of(r * TM, TM), TM), :].T
            return 0

        lax.fori_loop(0, nt, prep, 0)

    @pl.when((c == 1) & (le + 1 < n_e))
    def _():
        loads(e + 1, 1 - slot, True)

    @pl.when((c == 2) & (le > 0))
    def _():
        outputs(e - 1, le - 1, False)

    @pl.when(nt == 0)
    def _():
        gxs[...] = jnp.zeros_like(gxs)
        gds[...] = jnp.zeros_like(gds)

    nt_dims = (((1,), (1,)), ((), ()))
    tn_dims = (((0,), (0,)), ((), ()))

    def tile(r, n_tile, own):
        rows = pl.ds(pl.multiple_of(r * TM, TM), n_tile * TM)
        x = xbuf[slot, rows, :]
        d_o = dobuf[slot, rows, :]
        hg = jnp.dot(x, wg_ref[...], preferred_element_type=f32).astype(bf16).astype(f32)
        hu = jnp.dot(x, wu_ref[...], preferred_element_type=f32).astype(bf16).astype(f32)
        da = lax.dot_general(d_o, wd_ref[...], nt_dims, preferred_element_type=f32).astype(bf16).astype(f32)
        sig = jax.nn.sigmoid(hg)
        silu = hg * sig
        act = (silu * hu).astype(bf16)
        dhu = (da * silu).astype(bf16)
        dhg = (da * hu * sig * (1.0 + hg * (1.0 - sig))).astype(bf16)
        both = jnp.concatenate([dhg, dhu], axis=1)
        if own:
            new = c == 0
            o_acc[rows, :] = jnp.where(new, 0.0, o_acc[rows, :]) + jnp.dot(act, wd_ref[...], preferred_element_type=f32)
            w_both = jnp.concatenate([wg_ref[...], wu_ref[...]], axis=1)
            dx_acc[rows, :] = jnp.where(new, 0.0, dx_acc[rows, :]) + lax.dot_general(both, w_both, nt_dims, preferred_element_type=f32)
        xtr = xt[r] if n_tile == 1 else jnp.concatenate([xt[r + i] for i in range(n_tile)], axis=1)
        gxs[...] = jnp.where(r == 0, 0.0, gxs[...]) + jnp.dot(xtr, both, preferred_element_type=f32)
        gds[...] = jnp.where(r == 0, 0.0, gds[...]) + lax.dot_general(act, d_o, tn_dims, preferred_element_type=f32)

    def run(lo, n, own):
        pairs = lax.div(n, 2)

        def pair(i, _):
            tile(lo + 2 * i, 2, own)
            return 0

        def single(i, _):
            tile(lo + 2 * pairs + i, 1, own)
            return 0

        lax.fori_loop(0, pairs, pair, 0)
        lax.fori_loop(0, n - 2 * pairs, single, 0)

    run(0, nt_own, True)
    run(nt_own, nt - nt_own, False)
    gg_ref[...] = gxs[:, :CF].astype(bf16)
    gu_ref[...] = gxs[:, CF:].astype(bf16)
    gd_ref[...] = gds[...].astype(bf16)

    @pl.when(c == n_chunk - 1)
    def _():
        def cast(r, _):
            rows = pl.ds(pl.multiple_of(r * TM, TM), TM)
            ost[rows, :] = o_acc[rows, :].astype(bf16)
            dxst[rows, :] = dx_acc[rows, :].astype(bf16)
            return 0

        lax.fori_loop(0, nt_own, cast, 0)
        outputs(e, le, True)

        @pl.when(le + 1 == n_e)
        def _():
            outputs(e, le, False)


def run_experts(e0, n_e, cnt, soff, off, order, x_src, dy_src, seg_cap, w_gate, w_up, w_down, prev):
    n_src, cap, width = dy_src.shape
    n_loc = w_gate.shape[0]
    n_own = n_src // 2
    ff = w_gate.shape[2]
    n_chunk = ff // CF
    own_cap = n_own * seg_cap
    bf16 = jnp.bfloat16
    f32 = jnp.float32
    col_spec = pl.BlockSpec((None, width, CF), lambda i, c, cnt, soff, off, order: (order[e0 + i], 0, c))
    row_spec = pl.BlockSpec((None, CF, width), lambda i, c, cnt, soff, off, order: (order[e0 + i], c, 0))
    any_spec = pl.BlockSpec(memory_space=pl.ANY)
    first = prev is None
    if first:
        prev = (jnp.zeros((8, 128), bf16),) * 3
    out_shape = (
        jax.ShapeDtypeStruct((n_loc, width, ff), bf16),
        jax.ShapeDtypeStruct((n_loc, width, ff), bf16),
        jax.ShapeDtypeStruct((n_loc, ff, width), bf16),
    ) + (jax.ShapeDtypeStruct((2, n_e, seg_cap, width), bf16),) * n_own
    rows_est = n_e * cap // 2
    n_in = 10
    return pl.pallas_call(
        functools.partial(expert_kernel, e0, n_src, n_own, n_chunk),
        out_shape=out_shape,
        grid_spec=pltpu.PrefetchScalarGridSpec(
            num_scalar_prefetch=4,
            grid=(n_e, n_chunk),
            in_specs=[any_spec] * 3 + [col_spec, col_spec, row_spec] + [any_spec] * 3,
            out_specs=[col_spec, col_spec, row_spec] + [any_spec] * n_own,
            scratch_shapes=[
                pltpu.VMEM((2, cap, width), bf16),
                pltpu.VMEM((2, cap, width), bf16),
                pltpu.VMEM((cap // TM, width, TM), bf16),
                pltpu.VMEM((own_cap, width), f32),
                pltpu.VMEM((own_cap, width), f32),
                pltpu.VMEM((width, 2 * CF), f32),
                pltpu.VMEM((CF, width), f32),
                pltpu.VMEM((own_cap, width), bf16),
                pltpu.VMEM((own_cap, width), bf16),
                pltpu.SemaphoreType.DMA((3,)),
                pltpu.SemaphoreType.DMA((2,)),
            ],
        ),
        input_output_aliases={} if first else {n_in: 0, n_in + 1: 1, n_in + 2: 2},
        compiler_params=pltpu.CompilerParams(dimension_semantics=("arbitrary", "arbitrary"), vmem_limit_bytes=64000000),
        cost_estimate=pl.CostEstimate(flops=2 * 9 * rows_est * width * ff, bytes_accessed=n_e * width * ff * 12, transcendentals=0),
        name="experts",
    )(cnt, soff, off, order, *x_src, dy_src, w_gate, w_up, w_down, *prev)


def solution(mesh):
    n_dp, n_ep = mesh.shape["dp"], mesh.shape["ep"]
    n_dev = n_dp * n_ep
    all_axes = ("dp", "ep")

    def local_body(hidden, grad_out, expert_ids, norm_gain, w_router, w_gate, w_up, w_down):
        n_tok, width = hidden.shape
        n_exp = w_router.shape[1]
        n_loc = n_exp // n_ep
        capacity = 4 * n_tok // n_exp
        total_tok = n_tok * n_dev
        f32 = jnp.float32
        d_ix, e_ix = lax.axis_index("dp"), lax.axis_index("ep")

        dy_all = lax.all_gather(grad_out, all_axes, axis=0, tiled=True)

        x_f32 = hidden.astype(f32)
        inv_rms = lax.rsqrt(jnp.mean(x_f32 * x_f32, axis=-1, keepdims=True) + EPS)
        x_hat = x_f32 * inv_rms
        x_norm = (x_hat * norm_gain).astype(jnp.bfloat16)
        half = width // 2
        xa_all = lax.all_gather(x_norm[:, :half], all_axes, axis=0, tiled=True)
        xb_all = lax.all_gather(x_norm[:, half:], all_axes, axis=0, tiled=True)
        xn_f32 = x_norm.astype(f32)
        choice_hot = (expert_ids[:, :, None] == jnp.arange(n_exp, dtype=jnp.int32)).astype(f32)
        router_probs = jax.nn.softmax(jnp.dot(xn_f32, w_router, preferred_element_type=f32), axis=-1)
        gate_vals = jnp.sum(router_probs[:, None, :] * choice_hot, axis=-1)

        flat_ids = expert_ids.reshape(-1)
        one_hot = (flat_ids[:, None] == jnp.arange(n_exp, dtype=jnp.int32)[None, :]).astype(jnp.int32)
        running = jnp.cumsum(one_hot, axis=0) - 1
        dest_rows = flat_ids * capacity + jnp.sum(running * one_hot, axis=1)
        counts = jnp.sum(one_hot, axis=0)
        tokens = lax.broadcasted_iota(f32, (n_tok, 2), 0).reshape(-1)
        pair = jnp.stack([tokens, gate_vals.reshape(-1)], axis=1)
        n_slot = n_exp * capacity
        owner_rows = n_loc * capacity
        padded = (counts + (SUB - 1)) // SUB * SUB
        per_owner = padded.reshape(n_ep, n_loc)
        seg_off = (jnp.cumsum(per_owner, axis=1) - per_owner + owner_rows * jnp.arange(n_ep, dtype=jnp.int32)[:, None]).reshape(-1)
        packed = jnp.sum((running + seg_off[None, :]) * one_hot, axis=1)
        slots = jnp.broadcast_to(jnp.array([-1.0, 0.0], f32), (n_slot, 2)).at[packed].set(pair, unique_indices=True)
        slot_tok = slots[:, 0]
        slot_gate = slots[:, 1]
        mine = jnp.concatenate([slot_tok, slot_gate, counts.astype(f32), jnp.sum(router_probs, axis=0), jnp.zeros((64,), f32)])
        table = lax.all_gather(mine, all_axes, axis=0, tiled=False)
        all_counts = table[:, 2 * n_slot:2 * n_slot + n_exp]
        route_stats = jnp.sum(table[:, 2 * n_slot:2 * n_slot + 2 * n_exp], axis=0)
        load_frac = route_stats[:n_exp] / (2 * total_tok)
        aux_loss = AUX_COEF * n_exp * jnp.sum(load_frac * route_stats[n_exp:] / total_tok)

        src_ids = [lax.rem(d_ix + k // n_ep, n_dp) * n_ep + lax.rem(e_ix + k % n_ep, n_ep) for k in range(n_dev)]
        mine_of = [lax.dynamic_index_in_dim(table, s, 0, keepdims=False) for s in src_ids]

        def cols(lo):
            part = jnp.stack([lax.dynamic_slice_in_dim(t, lo + e_ix * owner_rows, owner_rows, axis=0) for t in mine_of])
            return jnp.broadcast_to(part[..., None], (n_dev, owner_rows, 128))

        tok_col, gate_col = cols(0), cols(n_slot)
        cnt = jnp.stack([lax.dynamic_slice_in_dim(t, 2 * n_slot + e_ix * n_loc, n_loc, axis=0) for t in mine_of], axis=1).astype(jnp.int32)
        cnt = (cnt + (SUB - 1)) // SUB * SUB
        soff = jnp.cumsum(cnt, axis=0) - cnt
        off = jnp.concatenate([jnp.zeros((n_loc, 1), jnp.int32), jnp.cumsum(cnt, axis=1)], axis=1)
        n_rows = jnp.sum(cnt, axis=0)
        src_vec = jnp.stack(src_ids).astype(jnp.int32)
        dy_src, hot = gather_rows(src_vec, n_rows, dy_all, n_tok, owner_rows, tok=tok_col, gate=gate_col)
        xa_all, hot = lax.optimization_barrier((xa_all, hot))
        xa_src = gather_rows(src_vec, n_rows, xa_all, n_tok, owner_rows, hot=hot)
        xb_all, xa_src = lax.optimization_barrier((xb_all, xa_src))
        x_src = (xa_src, gather_rows(src_vec, n_rows, xb_all, n_tok, owner_rows, hot=hot))

        blocks = (all_counts.astype(jnp.int32) + (SUB - 1)) // SUB * SUB
        own_blocks = jnp.where(d_ix == 0, blocks[:n_ep], blocks[n_ep:])
        work = 3 * ((jnp.sum(own_blocks, axis=0) + (TM - 1)) // TM) + 6 * ((jnp.sum(blocks, axis=0) + (TM - 1)) // TM)
        work = work.reshape(n_ep, n_loc)
        place = jnp.arange(n_loc, dtype=jnp.int32)
        ahead = (work[:, None, :] > work[:, :, None]) | ((work[:, None, :] == work[:, :, None]) & (place[None, None, :] < place[None, :, None]))
        rank = jnp.sum(ahead.astype(jnp.int32), axis=2)
        my_rank = lax.dynamic_index_in_dim(rank, e_ix, 0, keepdims=False)
        turn = (my_rank[None, :] == place[:, None]).astype(jnp.int32)
        order = jnp.sum(turn * place[None, :], axis=1)

        def in_order(arr):
            return jnp.sum(turn[:, :, None] * arr[None], axis=1)

        cnt, soff, off = in_order(cnt), in_order(soff), in_order(off)

        prev = None
        backs = [[] for _ in range(n_ep)]
        e0 = 0
        for per in GROUP_SIZES:
            outs = run_experts(e0, per, cnt, soff, off, order, x_src, dy_src, capacity, w_gate, w_up, w_down, prev)
            prev = outs[:3]
            e0 += per
            for k in range(n_ep):
                sent = outs[3 + k]
                moved = sent
                if k > 0:
                    ring = [(i, (i + k) % n_ep) for i in range(n_ep)]
                    if e0 < n_loc:
                        moved = lax.ppermute(sent, "ep", ring)
                    else:
                        moved = (lax.ppermute(sent[0], "ep", ring), lax.ppermute(sent[1], "ep", ring))
                backs[k].append(moved)
        g_gate, g_up, g_down = prev
        back_rows = jnp.concatenate([b[0] for bk in backs for b in bk], axis=0).reshape(n_slot, width)
        d_back = jnp.concatenate([b[1] for bk in backs for b in bk], axis=0).reshape(n_slot, width)
        owner = dest_rows // owner_rows
        back_ix = (lax.rem(e_ix - owner + n_ep, n_ep) * owner_rows + jnp.sum(one_hot * rank.reshape(1, -1), axis=1) * capacity + lax.rem(dest_rows, capacity)).reshape(n_tok, 2)

        def picks(rows):
            return [rows.at[back_ix[:, j]].get(mode="promise_in_bounds").astype(f32) for j in range(2)]

        picked = picks(back_rows)
        out_hidden = (x_f32 + (gate_vals[:, 0:1] * picked[0] + gate_vals[:, 1:2] * picked[1])).astype(jnp.bfloat16)
        dy_f32 = grad_out.astype(f32)
        d_gates = jnp.stack([jnp.sum(dy_f32 * p, axis=-1) for p in picked], axis=1)
        d_xn_exp = picks(d_back)

        d_probs = jnp.sum(d_gates[:, :, None] * choice_hot, axis=1) + (AUX_COEF * n_exp / total_tok) * load_frac
        d_logits = router_probs * (d_probs - jnp.sum(router_probs * d_probs, axis=-1, keepdims=True))
        d_xnorm = jnp.einsum("te,de->td", d_logits, w_router) + d_xn_exp[0] + d_xn_exp[1]
        d_xnorm = d_xnorm.astype(jnp.bfloat16).astype(f32)
        scaled = d_xnorm * norm_gain
        grad_hidden = (inv_rms * (scaled - x_hat * jnp.mean(scaled * x_hat, axis=-1, keepdims=True)) + dy_f32).astype(jnp.bfloat16)
        small = jnp.concatenate([jnp.einsum("td,te->ed", xn_f32, d_logits), jnp.sum(d_xnorm * x_hat, axis=0)[None, :]], axis=0)
        small = jnp.sum(lax.all_gather(small, all_axes, axis=0, tiled=False), axis=0)
        grad_router, grad_gain = small[:n_exp].T, small[n_exp]
        return (out_hidden, aux_loss, grad_hidden, grad_gain, grad_router, g_gate, g_up, g_down)

    tok_spec = P(all_axes, None)
    w_spec = P("ep", None, None)
    return jax.shard_map(local_body, mesh=mesh, in_specs=(tok_spec, tok_spec, tok_spec, P(), P(), w_spec, w_spec, w_spec), out_specs=(tok_spec, P(), tok_spec, P(), P(), w_spec, w_spec, w_spec), check_vma=False)
```
